32 devices in a mesh: row: 8 (over z, core), col: 4 (over y, x).
Axes of the slice: x: 2, y: 2, z: 4, core: 2. Of those that a mesh axis runs over, the one named last changes fastest.
Arguments:
- grm_prior: float32 [1024, 1024], P('row', 'col'), may hold values from -0.6 to 0.6
- dosage_now: bfloat16 [1024, 4096], P('row', 'col'), may hold values from 0 to 2
- mask_now: int32 [1024, 4096], P('row', 'col'), may hold values 0 or 1
- dosage_prev: bfloat16 [1024, 256], P('row'), may hold values from 0 to 2
- mask_prev: int32 [1024, 256], P('row'), may hold values 0 or 1
- expression: bfloat16 [1024, 20480], P('row', 'col'), may hold values from -18 to 18
Outputs:
- grm_total: float32 [1024, 1024], P('row', 'col')
- assoc_score: float32 [256, 20480], P('row', 'col')
The draws below stay inside these ranges and needn't reach their ends.
All inputs are finite; a program needn't handle non-finite values. No bound on the sum of `mask_now` or of `mask_prev` on one device may be relied on, other than what follows from the above.
Results may differ from the reference program's by a relative error of at most 0.0029.
Values may be sent and summed in bfloat16 or wider, within the bound.
A program may use at most 64 MiB of HBM per device.

```python
import math
import jax
import jax.numpy as jnp
from jax import lax

VARIANTS = 4096
ASSOC_VAR = 256
GENES = 20480
SAMPLES = 1024


def make_dosage(key, width):
    freq_key, draw_key = jax.random.split(key, 2)
    sample_ramp = (1.0 + 2.0 * jnp.arange(SAMPLES, dtype=jnp.float32) / (SAMPLES - 1)) / 3.0
    allele = jax.random.uniform(freq_key, (1, width), jnp.float32, 0.1, 0.5)
    base_draw = jax.random.uniform(draw_key, (SAMPLES, width), jnp.float32)
    return (4.0 * allele * base_draw * sample_ramp[:, None]).astype(jnp.bfloat16)


def draw_dosage_now(key, part):
    return make_dosage(jax.random.fold_in(key, 11), VARIANTS)


def draw_dosage_prev(key, part):
    return make_dosage(jax.random.fold_in(key, 23), ASSOC_VAR)


def draw_expression(key, part):
    inner_key = jax.random.fold_in(key, 37)
    noise_key = jax.random.fold_in(inner_key, 0)
    sample_ramp = 1.0 + 2.0 * jnp.arange(SAMPLES, dtype=jnp.float32) / (SAMPLES - 1)
    values = jnp.clip(jax.random.normal(noise_key, (SAMPLES, GENES), jnp.float32), -6.0, 6.0)
    return (values * sample_ramp[:, None]).astype(jnp.bfloat16)


def place_ends(array, rng, smallest, largest):
    longest = array.shape.index(max(array.shape))
    spots = []
    for shift in (0, 1):
        where = [jax.random.randint(jax.random.fold_in(rng, axis), (), 0, length) for axis, length in enumerate(array.shape)]
        where[longest] = (where[longest] + shift) % array.shape[longest]
        spots.append(tuple(where))
    return array.at[spots[0]].set(smallest).at[spots[1]].set(largest)


def levels(own_key, extent, cuts, low, largest):
    gain, own = 1.0, jax.random.fold_in(own_key, 6)
    for dim, blocks in cuts:
        steps = jnp.exp(jax.random.uniform(jax.random.fold_in(own, dim), (blocks,), jnp.float32, low / len(cuts), largest / len(cuts)))
        gain = gain * jnp.repeat(steps, extent[dim] // blocks).reshape([-1 if axis == dim else 1 for axis in range(len(extent))])
    return gain


def gaussian(own_key, extent, scale, reach, cuts=(), kind=jnp.bfloat16):
    values = scale * jax.random.normal(own_key, extent, jnp.float32)
    if cuts:
        values = values * levels(own_key, extent, cuts, -0.22, 0.18)
    return jnp.clip(values, -reach, reach).astype(kind)


def setup_inputs(seed: int = 0) -> dict:
    key_list = jax.random.split(jax.random.key(seed), 7)
    grm_prior = gaussian(key_list[0], (SAMPLES, SAMPLES), 0.1, 0.6, ((0, 8), (1, 4)), jnp.float32)
    dosage_now = draw_dosage_now(jax.random.fold_in(key_list[6], 71), 0)
    mask_now = place_ends((jax.random.randint(key_list[2], (SAMPLES, VARIANTS), 0, 10) < 9).astype(jnp.int32), jax.random.fold_in(key_list[2], 1), 0, 1)
    dosage_prev = draw_dosage_prev(jax.random.fold_in(key_list[6], 71), 0)
    mask_prev = place_ends((jax.random.randint(key_list[4], (SAMPLES, ASSOC_VAR), 0, 10) < 9).astype(jnp.int32), jax.random.fold_in(key_list[4], 1), 0, 1)
    expression = draw_expression(jax.random.fold_in(key_list[6], 71), 0)
    return dict(grm_prior=grm_prior, dosage_now=dosage_now, mask_now=mask_now, dosage_prev=dosage_prev, mask_prev=mask_prev, expression=expression)


epsilon = 1e-05

def moments(dosage, present):
    values = dosage.astype(jnp.float32)
    weight = present.astype(jnp.float32)
    observed = jnp.maximum(lax.optimization_barrier(jnp.sum(weight, 0)), 1.0)
    centre = lax.optimization_barrier(jnp.sum(weight * values, 0)) / observed
    offset = weight * (values - centre)
    spread = lax.optimization_barrier(jnp.sum(offset * offset, 0)) / observed
    return (offset, spread)

def reference(grm_prior, dosage_now, mask_now, dosage_prev, mask_prev, expression):
    offset_now, spread_now = moments(dosage_now, mask_now)
    scaled = (offset_now * lax.rsqrt(spread_now + epsilon)).astype(jnp.bfloat16)
    wide = scaled.astype(jnp.float32)
    product = jnp.dot(wide, wide.T, precision=lax.Precision.HIGHEST, preferred_element_type=jnp.float32)
    grm_total = grm_prior + product / VARIANTS
    offset_prev, spread_prev = moments(dosage_prev, mask_prev)
    genotype = offset_prev.astype(jnp.bfloat16).astype(jnp.float32)
    traits = expression.astype(jnp.float32)
    cross_sum = lax.dot_general(genotype, traits, (((0,), (0,)), ((), ())), precision=lax.Precision.HIGHEST, preferred_element_type=jnp.float32)
    power = lax.optimization_barrier(jnp.sum(traits * traits, 0)) / SAMPLES
    assoc_score = cross_sum * lax.rsqrt(spread_prev + epsilon)[:, None] * lax.rsqrt(power + epsilon)[None, :] / math.sqrt(SAMPLES)
    return (grm_total, assoc_score)
```

```python
import functools
import math

import jax
import jax.numpy as jnp
from jax import lax
from jax.experimental import pallas as pl
from jax.experimental.pallas import tpu as pltpu
from jax.sharding import PartitionSpec as P

epsilon = 1e-05
MESH = pl.DeviceIdType.MESH


def kernel(nrow, ncol, prior_ref, dn_ref, mn_ref, dp_ref, mp_ref, ex_ref, grm_ref, out_ref,
           stat, statp, panels, gt, inv, own, psend, precv, lsend, lrecv, gown, gsend, grecv,
           st_s, st_r, sp_s, sp_r, pr_s, pr_r, ln_s, ln_r, pan_s, pan_r, dup_s, dup_r, gr_s, gr_r):
    f32, bf16 = jnp.float32, jnp.bfloat16
    r, c = lax.axis_index("row"), lax.axis_index("col")
    z, k = r // 2, r % 2
    nz = nrow // 2
    partner = 2 * z + 1 - k
    rows, width = dn_ref.shape
    wide = dp_ref.shape[1]
    genes = ex_ref.shape[1]
    part = wide // nrow
    samples = rows * nrow

    def copy(src, dst, ssem, rsem, **where):
        return pltpu.make_async_remote_copy(
            src_ref=src, dst_ref=dst, send_sem=ssem, recv_sem=rsem,
            device_id=where, device_id_type=MESH)

    barrier = pltpu.get_barrier_semaphore()
    for o in range(1, nrow):
        pl.semaphore_signal(barrier, inc=1, device_id={"row": (r + o) % nrow}, device_id_type=MESH)
    for o in range(1, ncol):
        pl.semaphore_signal(barrier, inc=1, device_id={"col": (c + o) % ncol}, device_id_type=MESH)

    def local(d_ref, m_ref, at, size):
        v, w = d_ref[...].astype(f32), m_ref[...].astype(f32)
        n = jnp.sum(w, 0, keepdims=True)
        s = jnp.sum(w * v, 0, keepdims=True)
        off = w * (v - s / jnp.maximum(n, 1.0))
        stat[r, :, at:at + size] = n
        stat[r, :, at + size:at + 2 * size] = s
        stat[r, :, at + 2 * size:at + 3 * size] = jnp.sum(off * off, 0, keepdims=True)

    local(dp_ref, mp_ref, 0, wide)
    local(dn_ref, mn_ref, 3 * wide, width)
    pl.semaphore_wait(barrier, nrow + ncol - 2)

    def stat_copy(buf, ssem, rsem, slot, peer):
        return copy(buf.at[slot], buf.at[slot], ssem.at[peer], rsem.at[slot], row=peer)

    for o in range(1, nrow):
        stat_copy(stat, st_s, st_r, r, (r + o) % nrow).start()

    chunk = genes // 4
    for j in range(4):
        e = ex_ref[:, j * chunk:(j + 1) * chunk].astype(f32)
        statp[r, :, j * chunk:(j + 1) * chunk] = jnp.sum(e * e, 0, keepdims=True)
    for o in range(1, nrow):
        stat_copy(stat, st_s, st_r, (r + o) % nrow, (r + o) % nrow).wait_recv()

    def combine(at, size):
        n = [stat[q, :, at:at + size] for q in range(nrow)]
        s = [stat[q, :, at + size:at + 2 * size] for q in range(nrow)]
        observed = jnp.maximum(functools.reduce(jnp.add, n), 1.0)
        centre = functools.reduce(jnp.add, s) / observed
        second = jnp.zeros_like(centre)
        for q in range(nrow):
            gap = s[q] / jnp.maximum(n[q], 1.0) - centre
            second = second + (stat[q, :, at + 2 * size:at + 3 * size] + n[q] * gap * gap)
        return centre, lax.rsqrt(second / observed + epsilon)

    centre, scale = combine(0, wide)
    geno = mp_ref[...].astype(f32) * (dp_ref[...].astype(f32) - centre)
    geno = jnp.transpose(geno).astype(bf16)
    for d in range(nz):
        for q in range(2):
            gt[q, d * part:(d + 1) * part, :] = geno[(2 * d + q) * part:(2 * d + q + 1) * part, :]
    inv[...] = jnp.transpose(jnp.broadcast_to(scale, (rows, wide)))

    centre, scale = combine(3 * wide, width)
    panels[r] = (mn_ref[...].astype(f32) * (dn_ref[...].astype(f32) - centre) * scale).astype(bf16)

    def panel(slot, step):
        return copy(panels.at[slot], panels.at[slot], pan_s.at[slot], pan_r.at[slot],
                    row=r + 2 * step)

    def panel_back(slot):
        return copy(panels.at[slot], panels.at[slot], pan_s.at[nrow + slot], pan_r.at[slot],
                    row=r - 2)

    def dup(slot):
        return copy(panels.at[slot], panels.at[slot], dup_s.at[slot], dup_r.at[slot], row=partner)

    @pl.when(z < nz - 1)
    def _():
        panel(r, 1).start()

    @pl.when(z > 0)
    def _():
        panel_back(r).start()

    dup(r).start()

    other = gt[1 - k]
    for j in range(4):
        cols = slice(j * chunk, (j + 1) * chunk)
        psend[:, cols] = jnp.dot(other, ex_ref[:, cols], preferred_element_type=f32)

    def block(d):
        return pl.ds(pl.multiple_of(d * part, part), part)

    def pair(d):
        return copy(psend.at[block(d)], precv.at[block(d)], pr_s.at[d], pr_r.at[d], row=partner)

    order = [jnp.where(z < nz // 2, nz - 1 - i, i) for i in range(nz)]
    for i in range(nz):
        pair(order[i]).start()
    for o in range(1, nrow):
        stat_copy(statp, sp_s, sp_r, r, (r + o) % nrow).start()
    mine = gt[k]
    for j in range(4):
        cols = slice(j * chunk, (j + 1) * chunk)
        own[:, cols] = jnp.dot(mine, ex_ref[:, cols], preferred_element_type=f32)

    def line(d):
        target = jnp.where(d > z, z + 1, z - 1)
        slot = jnp.where(d == z - 1, nz, d)
        return copy(lsend.at[d], lrecv.at[slot], ln_s.at[d], ln_r.at[slot],
                    row=jnp.clip(2 * target + k, 0, nrow - 1))

    def line_wait(slot):
        copy(lsend.at[0], lrecv.at[slot], ln_s.at[0], ln_r.at[slot], row=partner).wait_recv()

    def cross_step(d):
        @pl.when(d != z)
        def _():
            pair(d).wait_recv()
            has = jnp.logical_or(jnp.logical_and(d > z, z > 0), jnp.logical_and(d < z, z < nz - 1))

            @pl.when(has)
            def _():
                line_wait(d)
                lsend[d] = (own[block(d), :] + precv[block(d), :] + lrecv[d].astype(f32)).astype(bf16)

            @pl.when(jnp.logical_not(has))
            def _():
                lsend[d] = (own[block(d), :] + precv[block(d), :]).astype(bf16)

            line(d).start()

    def gram(src, q):
        return copy(gsend.at[q], grecv.at[src], gr_s.at[q], gr_r.at[src], col=q)

    def gram_step(zz):
        dup(2 * zz + 1 - k).wait_recv()
        both = panels[pl.ds(2 * zz, 2)].reshape(2 * rows, width)
        value = lax.dot_general(panels[r], both, (((1,), (1,)), ((), ())), preferred_element_type=f32)

        @pl.when(zz == c)
        def _():
            gown[...] = value

        @pl.when(zz != c)
        def _():
            gsend[zz] = value
            gram(c, zz).start()

    def pan_wait(slot):
        copy(panels.at[slot], panels.at[slot], pan_s.at[slot], pan_r.at[slot], row=partner).wait_recv()

    cross_step(order[0])
    for t in range(1, nz):
        @pl.when(z - t >= 0)
        def _():
            slot = r - 2 * t
            pan_wait(slot)

            @pl.when(z < nz - 1)
            def _():
                panel(slot, 1).start()

            dup(slot).start()

        @pl.when(z + t < nz)
        def _():
            slot = r + 2 * t
            pan_wait(slot)

            @pl.when(z > 0)
            def _():
                panel_back(slot).start()

            dup(slot).start()

        if t == 1:
            gram_step(z)
        cross_step(order[t])

        @pl.when(z - t >= 0)
        def _():
            gram_step(z - t)

        @pl.when(z + t < nz)
        def _():
            gram_step(z + t)

    pair(z).wait_recv()
    power = statp[r]
    for o in range(1, nrow):
        q = (r + o) % nrow
        stat_copy(statp, sp_s, sp_r, q, q).wait_recv()
        power = power + statp[q]
    power = lax.rsqrt(power / samples + epsilon) / math.sqrt(samples)
    scale = inv[block(r), 0:1]

    @pl.when(z > 0)
    def _():
        line_wait(z)
        own[block(z), :] = own[block(z), :] + lrecv[z].astype(f32)

    @pl.when(z < nz - 1)
    def _():
        line_wait(nz)
        own[block(z), :] = own[block(z), :] + lrecv[nz].astype(f32)

    out_ref[...] = (own[block(z), :] + precv[block(z), :]) * scale * power

    total = gown[...]
    for o in range(1, ncol):
        src = (c + o) % ncol
        gram(src, src).wait_recv()
        total = total + grecv[src]
    grm_ref[...] = prior_ref[...] + total / (width * ncol)

    for o in range(1, nrow):
        q = (r + o) % nrow
        stat_copy(stat, st_s, st_r, r, q).wait_send()
        stat_copy(statp, sp_s, sp_r, r, q).wait_send()
    for d in range(nz):
        pair(d).wait_send()
        dup(2 * d + k).wait_send()

        @pl.when(d != z)
        def _():
            line(d).wait_send()

        @pl.when(jnp.logical_and(d <= z, z < nz - 1))
        def _():
            panel(2 * d + k, 1).wait_send()

        @pl.when(jnp.logical_and(d >= z, z > 0))
        def _():
            panel_back(2 * d + k).wait_send()
    for o in range(1, ncol):
        gram(c, (c + o) % ncol).wait_send()


def body(nrow, ncol, prior, dn, mn, dp, mp, ex):
    f32, bf16 = jnp.float32, jnp.bfloat16
    rows, width = dn.shape
    wide, genes = dp.shape[1], ex.shape[1]
    nz, part = nrow // 2, wide // nrow
    dma = pltpu.SemaphoreType.DMA
    scratch = [
        pltpu.VMEM((nrow, 1, 3 * (width + wide)), f32),
        pltpu.VMEM((nrow, 1, genes), f32),
        pltpu.VMEM((nrow, rows, width), bf16),
        pltpu.VMEM((2, nz * part, rows), bf16),
        pltpu.VMEM((wide, rows), f32),
        pltpu.VMEM((nz * part, genes), f32),
        pltpu.VMEM((nz * part, genes), f32),
        pltpu.VMEM((nz * part, genes), f32),
        pltpu.VMEM((nz, part, genes), bf16),
        pltpu.VMEM((nz + 1, part, genes), bf16),
        pltpu.VMEM(prior.shape, f32),
        pltpu.VMEM((ncol,) + prior.shape, f32),
        pltpu.VMEM((ncol,) + prior.shape, f32),
        dma((nrow,)), dma((nrow,)), dma((nrow,)), dma((nrow,)),
        dma((nz,)), dma((nz,)), dma((nz,)), dma((nz + 1,)),
        dma((2 * nrow,)), dma((nrow,)), dma((nrow,)), dma((nrow,)),
        dma((ncol,)), dma((ncol,)),
    ]
    vmem = pl.BlockSpec(memory_space=pltpu.VMEM)
    return pl.pallas_call(
        functools.partial(kernel, nrow, ncol),
        out_shape=(jax.ShapeDtypeStruct(prior.shape, f32), jax.ShapeDtypeStruct((part, genes), f32)),
        in_specs=[vmem] * 6,
        out_specs=(vmem, vmem),
        scratch_shapes=scratch,
        compiler_params=pltpu.CompilerParams(
            collective_id=0, has_side_effects=True, vmem_limit_bytes=66_000_000),
    )(prior, dn, mn, dp, mp, ex)


def solution(mesh):
    spec = P("row", "col")
    only = P("row", None)
    return jax.shard_map(
        functools.partial(body, mesh.shape["row"], mesh.shape["col"]),
        mesh=mesh, in_specs=(spec, spec, spec, only, only, spec), out_specs=(spec, spec),
        check_vma=False)
```

```python
import functools
import math

import jax
import jax.numpy as jnp
from jax import lax
from jax.experimental import pallas as pl
from jax.experimental.pallas import tpu as pltpu
from jax.sharding import PartitionSpec as P

epsilon = 1e-05
MESH = pl.DeviceIdType.MESH


HALVES = 2


def kernel(nrow, ncol, dn_hbm, mn_hbm, dp_hbm, mp_hbm, ex_hbm, gram_ref, out_ref,
           dn_ref, mn_ref, dp_ref, mp_ref, ex_ref,
           statq, stat, pw, pws, pwr, panels, gt, inv, own, psend, precv, lsend, lrecv,
           gsend, grecv, in_s,
           sq_s, sq_r, st_s, st_r, pw_s, pw_r, pr_s, pr_r, ln_s, ln_r, pan_s, pan_r, dup_s, dup_r,
           gr_s, gr_r):
    f32, bf16 = jnp.float32, jnp.bfloat16
    r, c = lax.axis_index("row"), lax.axis_index("col")
    z, k = r // 2, r % 2
    nz = nrow // 2
    partner = 2 * z + 1 - k
    rows, width = dn_ref.shape
    wide = dp_ref.shape[1]
    genes = ex_ref.shape[1]
    part = wide // nrow
    half = genes // HALVES
    samples = rows * nrow
    first, last = z == 0, z == nz - 1
    inner = jnp.logical_and(z > 0, z < nz - 1)

    def copy(src, dst, ssem, rsem, **where):
        return pltpu.make_async_remote_copy(
            src_ref=src, dst_ref=dst, send_sem=ssem, recv_sem=rsem,
            device_id=where, device_id_type=MESH)

    barrier = pltpu.get_barrier_semaphore()
    for o in range(1, nrow):
        pl.semaphore_signal(barrier, inc=1, device_id={"row": (r + o) % nrow}, device_id_type=MESH)
    for o in range(1, ncol):
        pl.semaphore_signal(barrier, inc=1, device_id={"col": (c + o) % ncol}, device_id_type=MESH)
    fetch = [pltpu.make_async_copy(a, b, in_s.at[i]) for i, (a, b) in enumerate((
        (dp_hbm, dp_ref), (mp_hbm, mp_ref), (dn_hbm, dn_ref), (mn_hbm, mn_ref), (ex_hbm, ex_ref)))]
    for f in fetch:
        f.start()

    def local(d_ref, m_ref, buf, size):
        v, w = d_ref[...].astype(f32), m_ref[...].astype(f32)
        n = jnp.sum(w, 0, keepdims=True)
        s = jnp.sum(w * v, 0, keepdims=True)
        off = w * (v - s / jnp.maximum(n, 1.0))
        buf[r, :, 0:size] = n
        buf[r, :, size:2 * size] = s
        buf[r, :, 2 * size:3 * size] = jnp.sum(off * off, 0, keepdims=True)

    def stat_copy(buf, ssem, rsem, slot, peer):
        return copy(buf.at[slot], buf.at[slot], ssem.at[peer], rsem.at[slot], row=peer)

    def send_stats(buf, ssem, rsem):
        for o in range(1, nrow):
            stat_copy(buf, ssem, rsem, r, (r + o) % nrow).start()

    def wait_stats(buf, ssem, rsem):
        for o in range(1, nrow):
            q = (r + o) % nrow
            stat_copy(buf, ssem, rsem, q, q).wait_recv()

    fetch[0].wait()
    fetch[1].wait()
    local(dp_ref, mp_ref, statq, wide)
    pl.semaphore_wait(barrier, nrow + ncol - 2)
    send_stats(statq, sq_s, sq_r)
    fetch[2].wait()
    fetch[3].wait()
    local(dn_ref, mn_ref, stat, width)
    send_stats(stat, st_s, st_r)
    fetch[4].wait()
    chunk = genes // 4
    for j in range(4):
        e = ex_ref[:, j * chunk:(j + 1) * chunk].astype(f32)
        pw[0, :, j * chunk:(j + 1) * chunk] = jnp.sum(e * e, 0, keepdims=True)
    pw_pair = copy(pw.at[0], pw.at[1], pw_s.at[0], pw_r.at[0], row=partner)
    pw_pair.start()

    def combine(buf, size):
        n = [buf[q, :, 0:size] for q in range(nrow)]
        s = [buf[q, :, size:2 * size] for q in range(nrow)]
        observed = jnp.maximum(functools.reduce(jnp.add, n), 1.0)
        centre = functools.reduce(jnp.add, s) / observed
        second = jnp.zeros_like(centre)
        for q in range(nrow):
            gap = s[q] / jnp.maximum(n[q], 1.0) - centre
            second = second + (buf[q, :, 2 * size:3 * size] + n[q] * gap * gap)
        return centre, lax.rsqrt(second / observed + epsilon)

    wait_stats(statq, sq_s, sq_r)
    centre, scale = combine(statq, wide)
    geno = mp_ref[...].astype(f32) * (dp_ref[...].astype(f32) - centre)
    geno = jnp.transpose(geno).astype(bf16)
    for d in range(nz):
        for q in range(2):
            gt[q, d * part:(d + 1) * part, :] = geno[(2 * d + q) * part:(2 * d + q + 1) * part, :]

    def pair(d, h):
        return copy(psend.at[d, h], precv.at[d, h], pr_s.at[d, h], pr_r.at[d, h], row=partner)

    def products(lhs, dst, h):
        cols = slice(h * half, (h + 1) * half)
        value = jnp.dot(lhs, ex_ref[:, cols], preferred_element_type=f32)
        for d in range(nz):
            dst[d, h] = value[d * part:(d + 1) * part, :]

    other = gt[1 - k]
    outward = sorted(range(nz), key=lambda d: min(d, nz - 1 - d))
    for h in range(HALVES):
        products(other, psend, h)
        for d in outward:
            pair(d, h).start()

    def panel(slot):
        return copy(panels.at[slot], panels.at[slot], pan_s.at[slot], pan_r.at[slot], row=r + 2)

    def panel_back(slot):
        return copy(panels.at[slot], panels.at[slot], pan_s.at[nrow + slot], pan_r.at[slot],
                    row=r - 2)

    def dup(slot):
        return copy(panels.at[slot], panels.at[slot], dup_s.at[slot], dup_r.at[slot], row=partner)

    def pan_wait(slot):
        copy(panels.at[slot], panels.at[slot], pan_s.at[slot], pan_r.at[slot], row=partner).wait_recv()

    wait_stats(stat, st_s, st_r)
    centre, scale_now = combine(stat, width)
    panels[r] = (mn_ref[...].astype(f32) * (dn_ref[...].astype(f32) - centre) * scale_now).astype(bf16)

    @pl.when(jnp.logical_not(last))
    def _():
        panel(r).start()

    @pl.when(jnp.logical_not(first))
    def _():
        panel_back(r).start()

    dup(r).start()
    mine = gt[k]
    for h in range(HALVES):
        products(mine, own, h)
    inv[...] = jnp.transpose(jnp.broadcast_to(scale, (rows, wide)))

    pw_pair.wait()
    pw[0] = pw[0] + pw[1]

    def pw_line(way):
        return copy(pws.at[way], pwr.at[way], pw_s.at[1 + way], pw_r.at[1 + way],
                    row=jnp.clip(r + 2 - 4 * way, 0, nrow - 1))

    def line(d, h, way):
        if way == 0:
            slot = d
        else:
            slot = jnp.where(d == z - 1, nz, d)
        return copy(lsend.at[d, h], lrecv.at[slot, h], ln_s.at[d, h], ln_r.at[slot, h],
                    row=jnp.clip(r + 2 - 4 * way, 0, nrow - 1))

    def line_wait(slot, h):
        copy(lsend.at[0, h], lrecv.at[slot, h], ln_s.at[0, h], ln_r.at[slot, h], row=partner).wait_recv()

    def start_line(d, h, way):
        pair(d, h).wait_recv()
        lsend[d, h] = (own[d, h] + precv[d, h]).astype(bf16)
        line(d, h, way).start()

    def pass_line(d, h, way):
        pair(d, h).wait_recv()
        value = own[d, h] + precv[d, h]
        line_wait(d, h)
        lsend[d, h] = (value + lrecv[d, h].astype(f32)).astype(bf16)
        line(d, h, way).start()

    for way, end in ((0, first), (1, last)):
        @pl.when(end)
        def _():
            pws[way] = pw[0]
            pw_line(way).start()
            for h in range(HALVES):
                for d in (range(nz - 1, 0, -1) if way == 0 else range(nz - 1)):
                    start_line(d, h, way)

    def gram(src, q):
        return copy(gsend.at[q], grecv.at[src], gr_s.at[q], gr_r.at[src], col=q)

    def gram_step(zz):
        dup(2 * zz + 1 - k).wait_recv()
        both = panels[pl.ds(2 * zz, 2)].reshape(2 * rows, width)
        value = lax.dot_general(panels[r], both, (((1,), (1,)), ((), ())), preferred_element_type=f32)

        @pl.when(zz == c)
        def _():
            gram_ref[...] = value

        @pl.when(zz != c)
        def _():
            gsend[zz] = value
            gram(c, zz).start()

    def hop(t):
        @pl.when(z - t >= 0)
        def _():
            slot = r - 2 * t
            pan_wait(slot)

            @pl.when(jnp.logical_not(last))
            def _():
                panel(slot).start()

            dup(slot).start()

        @pl.when(z + t < nz)
        def _():
            slot = r + 2 * t
            pan_wait(slot)

            @pl.when(jnp.logical_not(first))
            def _():
                panel_back(slot).start()

            dup(slot).start()

    def near(t):
        if t == 0:
            gram_step(z)
            return

        @pl.when(z - t >= 0)
        def _():
            gram_step(z - t)

        @pl.when(z + t < nz)
        def _():
            gram_step(z + t)

    low = jnp.logical_and(inner, z < nz // 2)
    high = jnp.logical_and(inner, z >= nz // 2)

    def pass_pw(way):
        copy(pws.at[way], pwr.at[way], pw_s.at[1 + way], pw_r.at[1 + way], row=partner).wait_recv()
        pws[way] = pw[0] + pwr[way]
        pw_line(way).start()

    def pass_key(m, way, when):
        if m == 0:
            @pl.when(when)
            def _():
                pass_pw(way)

        @pl.when(jnp.logical_and(when, (z < nz - 1 - m) if way == 0 else (z > m)))
        def _():
            for h in range(HALVES):
                pass_line(nz - 1 - m if way == 0 else m, h, way)

    for m in range(nz - 1):
        hop(m + 1)
        pass_key(m, 0, low)
        pass_key(m, 1, high)
        near(m)
    for m in range(nz - 1):
        pass_key(m, 1, low)
        pass_key(m, 0, high)
    near(nz - 1)

    total = gram_ref[...]
    for o in range(1, ncol):
        src = (c + o) % ncol
        gram(src, src).wait_recv()
        total = total + grecv[src]
    gram_ref[...] = total

    def pw_wait(way):
        copy(pws.at[way], pwr.at[way], pw_s.at[1 + way], pw_r.at[1 + way], row=partner).wait_recv()
        pw[0] = pw[0] + pwr[way]

    @pl.when(first)
    def _():
        pw_wait(1)

    @pl.when(last)
    def _():
        pw_wait(0)

    @pl.when(inner)
    def _():
        pw[0] = pw[0] + pwr[0] + pwr[1]

    power = lax.rsqrt(pw[0] / samples + epsilon) / math.sqrt(samples)
    scale = inv[pl.ds(pl.multiple_of(r * part, part), part), 0:1]
    for h in range(HALVES):
        pair(z, h).wait_recv()

        @pl.when(z > 0)
        def _():
            line_wait(z, h)
            own[z, h] = own[z, h] + lrecv[z, h].astype(f32)

        @pl.when(z < nz - 1)
        def _():
            line_wait(nz, h)
            own[z, h] = own[z, h] + lrecv[nz, h].astype(f32)

        out_ref[:, h * half:(h + 1) * half] = (
            (own[z, h] + precv[z, h]) * scale * power[:, h * half:(h + 1) * half])


    @pl.when(jnp.logical_not(last))
    def _():
        pw_line(0).wait_send()

    @pl.when(jnp.logical_not(first))
    def _():
        pw_line(1).wait_send()

    for o in range(1, nrow):
        q = (r + o) % nrow
        stat_copy(statq, sq_s, sq_r, r, q).wait_send()
        stat_copy(stat, st_s, st_r, r, q).wait_send()
    for d in range(nz):
        dup(2 * d + k).wait_send()
        for h in range(HALVES):
            pair(d, h).wait_send()

            @pl.when(d > z)
            def _():
                line(d, h, 0).wait_send()

            @pl.when(d < z)
            def _():
                line(d, h, 1).wait_send()

        @pl.when(jnp.logical_and(d <= z, z < nz - 1))
        def _():
            panel(2 * d + k).wait_send()

        @pl.when(jnp.logical_and(d >= z, z > 0))
        def _():
            panel_back(2 * d + k).wait_send()
    for o in range(1, ncol):
        gram(c, (c + o) % ncol).wait_send()


def finish(variants, prior_hbm, gram_hbm, cross_hbm, grm_ref, out_ref, prior_ref, gram_ref, in_s):
    fetch = [pltpu.make_async_copy(a, b, in_s.at[i]) for i, (a, b) in enumerate((
        (cross_hbm, out_ref), (prior_hbm, prior_ref), (gram_hbm, gram_ref)))]
    for f in fetch:
        f.start()
    fetch[1].wait()
    fetch[2].wait()
    grm_ref[...] = prior_ref[...] + gram_ref[...] / variants
    fetch[0].wait()


def body(nrow, ncol, prior, dn, mn, dp, mp, ex):
    f32, bf16 = jnp.float32, jnp.bfloat16
    rows, width = dn.shape
    wide, genes = dp.shape[1], ex.shape[1]
    nz, part, half = nrow // 2, wide // nrow, genes // HALVES
    dma = pltpu.SemaphoreType.DMA
    scratch = [pltpu.VMEM(a.shape, a.dtype) for a in (dn, mn, dp, mp, ex)] + [
        pltpu.VMEM((nrow, 1, 3 * wide), f32),
        pltpu.VMEM((nrow, 1, 3 * width), f32),
        pltpu.VMEM((2, 1, genes), f32),
        pltpu.VMEM((2, 1, genes), f32),
        pltpu.VMEM((2, 1, genes), f32),
        pltpu.VMEM((nrow, rows, width), bf16),
        pltpu.VMEM((2, nz * part, rows), bf16),
        pltpu.VMEM((wide, rows), f32),
        pltpu.VMEM((nz, HALVES, part, half), f32),
        pltpu.VMEM((nz, HALVES, part, half), f32),
        pltpu.VMEM((nz, HALVES, part, half), f32),
        pltpu.VMEM((nz, HALVES, part, half), bf16),
        pltpu.VMEM((nz + 1, HALVES, part, half), bf16),
        pltpu.VMEM((ncol,) + prior.shape, f32),
        pltpu.VMEM((ncol,) + prior.shape, f32),
        dma((5,)),
        dma((nrow,)), dma((nrow,)), dma((nrow,)), dma((nrow,)), dma((3,)), dma((3,)),
        dma((nz, HALVES)), dma((nz, HALVES)), dma((nz, HALVES)), dma((nz + 1, HALVES)),
        dma((2 * nrow,)), dma((nrow,)), dma((nrow,)), dma((nrow,)),
        dma((ncol,)), dma((ncol,)),
    ]
    vmem = pl.BlockSpec(memory_space=pltpu.VMEM)
    hbm = pl.BlockSpec(memory_space=pltpu.HBM)
    gram, cross = pl.pallas_call(
        functools.partial(kernel, nrow, ncol),
        out_shape=(jax.ShapeDtypeStruct(prior.shape, f32), jax.ShapeDtypeStruct((part, genes), f32)),
        in_specs=[hbm] * 5,
        out_specs=(vmem,) * 2,
        scratch_shapes=scratch,
        compiler_params=pltpu.CompilerParams(
            collective_id=0, has_side_effects=True, vmem_limit_bytes=66000000),
    )(dn, mn, dp, mp, ex)
    return pl.pallas_call(
        functools.partial(finish, width * ncol),
        out_shape=(jax.ShapeDtypeStruct(prior.shape, f32), jax.ShapeDtypeStruct((part, genes), f32)),
        in_specs=[hbm] * 3,
        out_specs=(vmem,) * 2,
        scratch_shapes=[pltpu.VMEM(prior.shape, f32), pltpu.VMEM(prior.shape, f32), dma((3,))],
        compiler_params=pltpu.CompilerParams(vmem_limit_bytes=66000000),
    )(prior, gram, cross)


def solution(mesh):
    spec = P("row", "col")
    only = P("row", None)
    return jax.shard_map(
        functools.partial(body, mesh.shape["row"], mesh.shape["col"]),
        mesh=mesh, in_specs=(spec, spec, spec, only, only, spec), out_specs=(spec, spec),
        check_vma=False)
```
